32 devices in a mesh: ta: 4 (over z), sa: 8 (over y, x, core).
Axes of the slice: x: 2, y: 2, z: 4, core: 2. Of those that a mesh axis runs over, the one named last changes fastest.
Arguments:
- frames: float32 [16, 8, 512, 4096], P('ta', 'sa'), may hold values from -6 to 6
- taps: float32 [7], replicated, may hold values from 0.1 to 0.3
Outputs:
- columns: float32 [64, 16, 512, 512], P('sa', 'ta')
The draws below stay inside these ranges and needn't reach their ends.
All inputs are finite; a program needn't handle non-finite values.
Results may differ from the reference program's by a relative error of at most 0.00002.
Values sent between devices are 32-bit elements; how exact they have to be, the bound alone decides.
No kernel may reach another device: no remote copies, remote signals or barrier semaphores. Data moves between devices by JAX's collectives and lax.ppermute only.
A program may use at most 256 MiB of HBM per device.

```python
import jax
import jax.numpy as jnp
from jax import lax

NY = 4096
NX = 4096
TS = 512
TIME = 16
READERS = 8
STRIP = 512
TILES = 64
N_SA = 8


def level_of(rng, extent, cuts, low, high):
    gain = 1.0
    for axis_at, blocks in cuts:
        heights = jax.random.uniform(jax.random.fold_in(jax.random.fold_in(rng, 6), axis_at), (blocks,), jnp.float32, low / len(cuts), high / len(cuts))
        gain = gain * jnp.repeat(jnp.exp(heights), extent[axis_at] // blocks).reshape((-1,) + (1,) * (len(extent) - 1 - axis_at))
    return gain


def normal_values(stream_key, shape, deviation, limit, pieces=(), kind=jnp.bfloat16):
    result = deviation * jax.random.normal(stream_key, shape, jnp.float32)
    if pieces:
        result = result * level_of(stream_key, shape, pieces, -0.22, 0.18)
    return jnp.clip(result, -limit, limit).astype(kind)


def setup_inputs(seed: int = 0) -> dict:
    seeds = jax.random.split(jax.random.key(seed), 3)
    return {
        "frames": normal_values(seeds[0], (TIME, READERS, STRIP, NX), 1.0, 6.0, ((0, 4), (1, 8)), jnp.float32),
        "taps": jnp.clip(jax.random.uniform(seeds[1], (7,), jnp.float32, 0.1, 0.3), 0.1, 0.3),
    }


def reference(frames, taps):
    per_tile = TS // N_SA
    tile_rows = NY // TS
    tile_cols = NX // TS

    def one_row(index):
        piece = lax.dynamic_slice_in_dim(frames, index * per_tile, per_tile, 2)
        field = piece.transpose(0, 2, 1, 3).reshape(TIME, TS, NX)
        padded = jnp.pad(field, ((3, 3), (0, 0), (0, 0)))
        total = jnp.zeros_like(field)
        for offset in range(7):
            total = total + taps[offset] * padded[offset:offset + TIME]
        return total.reshape(TIME, TS, tile_cols, TS).transpose(2, 0, 1, 3)

    stacked = lax.map(one_row, jnp.arange(tile_rows, dtype=jnp.int32))
    return stacked.reshape(TILES, TIME, TS, TS)
```

```python
import functools
import math

import jax
import jax.numpy as jnp
from jax import lax
from jax.experimental import pallas as pl
from jax.experimental.pallas import tpu as pltpu
from jax.sharding import PartitionSpec as P


TS = 512
REACH = 3
LANES = 128
SUBLANES = 8
SHARES = (2, 3, 4, 5, 6, 6, 4, 2)


def chunk_bounds(width):
    units = width // LANES
    edges, seen = [0], 0
    for share in SHARES:
        seen += share
        edge = units * seen // sum(SHARES)
        if edge > edges[-1]:
            edges.append(edge)
    return [(a * LANES, b * LANES) for a, b in zip(edges, edges[1:])]


def pack_kernel(per_tile, frames_ref, first_ref, middle_ref, last_ref):
    steps = frames_ref.shape[0]
    for tile in range(first_ref.shape[0]):
        rows = pl.ds(tile * per_tile, per_tile)
        first_ref[tile, 0, 0] = frames_ref[0, 0, rows, :]
        for t in range(1, steps - 1):
            middle_ref[tile, 0, t - 1] = frames_ref[t, 0, rows, :]
        last_ref[tile, 0, 0] = frames_ref[steps - 1, 0, rows, :]


def pack_chunk(frames, readers, per_tile, span, start, width):
    steps, _, strip, columns = frames.shape
    tile_rows, groups = strip // per_tile, columns // span
    block = math.gcd(start, width)
    block = math.gcd(block, span) if groups > 1 else block

    def piece(depth):
        shape = (tile_rows, groups, depth, per_tile, width)
        spec = pl.BlockSpec(
            (tile_rows, 1, depth, per_tile, block), lambda g, i: (0, g, 0, 0, i)
        )
        return jax.ShapeDtypeStruct(shape, jnp.float32), spec

    pieces = [piece(1), piece(steps - 2), piece(1)]
    outs = pl.pallas_call(
        functools.partial(pack_kernel, per_tile),
        grid=(groups, width // block),
        out_shape=[p[0] for p in pieces],
        in_specs=[
            pl.BlockSpec(
                (steps, 1, strip, block),
                lambda g, i: (0, 0, 0, g * (span // block) + start // block + i),
            )
        ],
        out_specs=[p[1] for p in pieces],
        cost_estimate=pl.CostEstimate(
            flops=steps * strip * width * groups,
            bytes_accessed=8 * steps * strip * width * groups,
            transcendentals=0,
        ),
        name="pack",
    )(frames)
    return [o.reshape((readers,) + o.shape[2:]) for o in outs]


def smooth_kernel(readers, groups, taps_ref, *refs):
    first, middle, last, before_mid, before_last, after_first, after_mid = refs[:7]
    out_ref = refs[-1]
    steps = out_ref.shape[1]
    taps = [taps_ref[j] for j in range(2 * REACH + 1)]

    def body(group, carry):
        rows = pl.ds(pl.multiple_of(group * SUBLANES, SUBLANES), SUBLANES)
        for s in range(readers):
            field = [
                before_mid[s, 0, rows, :],
                before_mid[s, 1, rows, :],
                before_last[s, 0, rows, :],
                first[s, 0, rows, :],
                middle[s, 0, rows, :],
                middle[s, 1, rows, :],
                last[s, 0, rows, :],
                after_first[s, 0, rows, :],
                after_mid[s, 0, rows, :],
                after_mid[s, 1, rows, :],
            ]
            for t in range(steps):
                total = taps[0] * field[t]
                for j in range(1, 2 * REACH + 1):
                    total = total + taps[j] * field[t + j]
                at = group * (SUBLANES * readers) + s
                out_ref[0, t, pl.ds(at, SUBLANES, stride=readers), :] = total
        return carry

    lax.fori_loop(0, groups, body, 0)


def smooth_chunk(taps, pieces, out, out_shape, start, width):
    readers, _, per_tile, _ = pieces[0].shape
    steps = out_shape[1]
    offset = start // LANES
    per_row = TS // LANES

    def piece_spec(piece):
        return pl.BlockSpec(
            (readers, piece.shape[1], per_tile, LANES), lambda i: (0, 0, 0, i)
        )

    in_specs = [pl.BlockSpec(memory_space=pltpu.SMEM)] + [piece_spec(p) for p in pieces]
    operands = [taps, *pieces]
    aliases = {}
    if out is not None:
        in_specs.append(pl.BlockSpec(memory_space=pl.ANY))
        aliases = {len(operands): 0}
        operands.append(out)
    elements = readers * per_tile * width
    return pl.pallas_call(
        functools.partial(smooth_kernel, readers, per_tile // SUBLANES),
        grid=(width // LANES,),
        out_shape=jax.ShapeDtypeStruct(out_shape, jnp.float32),
        in_specs=in_specs,
        out_specs=pl.BlockSpec(
            (1, steps, TS, LANES),
            lambda i: ((i + offset) // per_row, 0, 0, (i + offset) % per_row),
        ),
        input_output_aliases=aliases,
        cost_estimate=pl.CostEstimate(
            flops=14 * steps * elements, bytes_accessed=14 * 4 * elements, transcendentals=0
        ),
        compiler_params=pltpu.CompilerParams(dimension_semantics=("arbitrary",)),
        name="smooth",
    )(*operands)


def on_device(frames, taps):
    steps, _, strip, columns = frames.shape
    readers = lax.axis_size("sa")
    count = lax.axis_size("ta")
    per_tile = TS // readers
    tile_rows = strip // per_tile
    owned = tile_rows * (columns // TS) // readers
    span = owned * TS
    out_shape = (owned, steps, TS, TS)
    up = [(i, i + 1) for i in range(count - 1)]
    down = [(i + 1, i) for i in range(count - 1)]
    swap = functools.partial(
        lax.all_to_all, axis_name="sa", split_axis=0, concat_axis=0, tiled=True
    )

    out = None
    for start, stop in chunk_bounds(span):
        first, middle, last = pack_chunk(frames, readers, per_tile, span, start, stop - start)
        middle = swap(middle)
        before_mid = lax.ppermute(middle, "ta", up)
        after_mid = lax.ppermute(middle, "ta", down)
        first = swap(first)
        after_first = lax.ppermute(first, "ta", down)
        last = swap(last)
        before_last = lax.ppermute(last, "ta", up)
        pieces = (first, middle, last, before_mid, before_last, after_first, after_mid)
        out = smooth_chunk(taps, pieces, out, out_shape, start, stop - start)
    return out


def solution(mesh):
    placed = (P("ta", "sa", None, None), P())

    return jax.shard_map(
        on_device, mesh=mesh, in_specs=placed, out_specs=P("sa", "ta", None, None), check_vma=False
    )
```

```python
import functools
import math

import jax
import jax.numpy as jnp
from jax import lax
from jax.experimental import pallas as pl
from jax.experimental.pallas import tpu as pltpu
from jax.sharding import PartitionSpec as P


TS = 512
REACH = 3
LANES = 128
SUBLANES = 8
EARLY = (2, 8)
LATE = (18, 4)


def chunk_bounds(width):
    units = width // LANES
    shares = EARLY + LATE
    edges = [units * sum(shares[:i]) // sum(shares) for i in range(len(shares) + 1)]
    bounds = [(a * LANES, b * LANES) for a, b in zip(edges, edges[1:])]
    early = [b for b in bounds[: len(EARLY)] if b[0] < b[1]]
    late = [b for b in bounds[len(EARLY) :] if b[0] < b[1]]
    return early, late


def weighted(taps, field, t):
    total = taps[0] * field[t]
    for j in range(1, 2 * REACH + 1):
        total = total + taps[j] * field[t + j]
    return total


def raw_kernel(frames_ref, up_ref, down_ref):
    steps = frames_ref.shape[0]
    for t in range(REACH):
        up_ref[t] = frames_ref[steps - REACH + t, 0]
        down_ref[t] = frames_ref[t, 0]


def raw_chunk(frames, span, start, width):
    steps, _, strip, columns = frames.shape
    groups = columns // span
    block = math.gcd(math.gcd(start, width), span)
    side = jax.ShapeDtypeStruct((REACH, strip, groups * width), jnp.float32)
    per_group = width // block
    elements = strip * groups * width
    return pl.pallas_call(
        raw_kernel,
        grid=(groups, per_group),
        out_shape=[side, side],
        in_specs=[
            pl.BlockSpec(
                (steps, 1, strip, block),
                lambda g, i: (0, 0, 0, g * (span // block) + start // block + i),
            )
        ],
        out_specs=[
            pl.BlockSpec((REACH, strip, block), lambda g, i: (0, 0, g * per_group + i))
        ]
        * 2,
        cost_estimate=pl.CostEstimate(
            flops=elements, bytes_accessed=4 * (steps + 2 * REACH) * elements, transcendentals=0
        ),
        name="raw",
    )(frames)


def early_kernel(per_tile, taps_ref, frames_ref, before_ref, after_ref, *refs):
    out_ref = refs[-1]
    steps = frames_ref.shape[0]
    taps = [taps_ref[j] for j in range(2 * REACH + 1)]

    def body(tile, carry):
        for group in range(per_tile // SUBLANES):
            at = pl.multiple_of(tile * per_tile + group * SUBLANES, SUBLANES)
            rows = pl.ds(at, SUBLANES)
            field = [before_ref[t, rows, :] for t in range(REACH)]
            field += [frames_ref[t, 0, rows, :] for t in range(steps)]
            field += [after_ref[t, rows, :] for t in range(REACH)]
            inside = pl.ds(group * SUBLANES, SUBLANES)
            for t in range(steps):
                out_ref[tile, 0, t, inside, :] = weighted(taps, field, t)
        return carry

    lax.fori_loop(0, out_ref.shape[0], body, 0)


def early_chunk(taps, frames, before, after, packed, shape, start, offset):
    steps, _, strip, columns = frames.shape
    tile_rows, groups, _, per_tile, _ = shape
    span = columns // groups
    width = before.shape[2] // groups
    per_group = width // LANES
    side = pl.BlockSpec((REACH, strip, LANES), lambda g, i: (0, 0, g * per_group + i))
    in_specs = [
        pl.BlockSpec(memory_space=pltpu.SMEM),
        pl.BlockSpec(
            (steps, 1, strip, LANES),
            lambda g, i: (0, 0, 0, g * (span // LANES) + start // LANES + i),
        ),
        side,
        side,
    ]
    operands = [taps, frames, before, after]
    aliases = {}
    if packed is not None:
        in_specs.append(pl.BlockSpec(memory_space=pl.ANY))
        aliases = {len(operands): 0}
        operands.append(packed)
    elements = strip * groups * width
    return pl.pallas_call(
        functools.partial(early_kernel, per_tile),
        grid=(groups, per_group),
        out_shape=jax.ShapeDtypeStruct(shape, jnp.float32),
        in_specs=in_specs,
        out_specs=pl.BlockSpec(
            (tile_rows, 1, steps, per_tile, LANES),
            lambda g, i: (0, g, 0, 0, offset // LANES + i),
        ),
        input_output_aliases=aliases,
        cost_estimate=pl.CostEstimate(
            flops=14 * steps * elements,
            bytes_accessed=4 * (2 * steps + 2 * REACH) * elements,
            transcendentals=0,
        ),
        name="early",
    )(*operands)


def place_kernel(readers, groups, piece_ref, *refs):
    out_ref = refs[-1]

    def body(group, carry):
        rows = pl.ds(pl.multiple_of(group * SUBLANES, SUBLANES), SUBLANES)
        for s in range(readers):
            at = group * (SUBLANES * readers) + s
            for t in range(out_ref.shape[1]):
                out_ref[0, t, pl.ds(at, SUBLANES, stride=readers), :] = piece_ref[s, t, rows, :]
        return carry

    lax.fori_loop(0, groups, body, 0)


def pack_kernel(per_tile, frames_ref, first_ref, middle_ref, last_ref):
    steps = frames_ref.shape[0]
    for tile in range(first_ref.shape[0]):
        rows = pl.ds(tile * per_tile, per_tile)
        first_ref[tile, 0, 0] = frames_ref[0, 0, rows, :]
        for t in range(1, steps - 1):
            middle_ref[tile, 0, t - 1] = frames_ref[t, 0, rows, :]
        last_ref[tile, 0, 0] = frames_ref[steps - 1, 0, rows, :]


def pack_chunk(frames, readers, per_tile, span, start, width):
    steps, _, strip, columns = frames.shape
    tile_rows, groups = strip // per_tile, columns // span
    block = math.gcd(start, width)
    block = math.gcd(block, span) if groups > 1 else block

    def piece(depth):
        shape = (tile_rows, groups, depth, per_tile, width)
        spec = pl.BlockSpec(
            (tile_rows, 1, depth, per_tile, block), lambda g, i: (0, g, 0, 0, i)
        )
        return jax.ShapeDtypeStruct(shape, jnp.float32), spec

    pieces = [piece(1), piece(steps - 2), piece(1)]
    outs = pl.pallas_call(
        functools.partial(pack_kernel, per_tile),
        grid=(groups, width // block),
        out_shape=[p[0] for p in pieces],
        in_specs=[
            pl.BlockSpec(
                (steps, 1, strip, block),
                lambda g, i: (0, 0, 0, g * (span // block) + start // block + i),
            )
        ],
        out_specs=[p[1] for p in pieces],
        cost_estimate=pl.CostEstimate(
            flops=steps * strip * width * groups,
            bytes_accessed=8 * steps * strip * width * groups,
            transcendentals=0,
        ),
        name="pack",
    )(frames)
    return [o.reshape((readers,) + o.shape[2:]) for o in outs]


def smooth_kernel(readers, groups, taps_ref, *refs):
    first, middle, last, before_mid, before_last, after_first, after_mid = refs[:7]
    out_ref = refs[-1]
    steps = out_ref.shape[1]
    taps = [taps_ref[j] for j in range(2 * REACH + 1)]

    def body(group, carry):
        rows = pl.ds(pl.multiple_of(group * SUBLANES, SUBLANES), SUBLANES)
        for s in range(readers):
            field = [
                before_mid[s, 0, rows, :],
                before_mid[s, 1, rows, :],
                before_last[s, 0, rows, :],
                first[s, 0, rows, :],
                middle[s, 0, rows, :],
                middle[s, 1, rows, :],
                last[s, 0, rows, :],
                after_first[s, 0, rows, :],
                after_mid[s, 0, rows, :],
                after_mid[s, 1, rows, :],
            ]
            for t in range(steps):
                at = group * (SUBLANES * readers) + s
                out_ref[0, t, pl.ds(at, SUBLANES, stride=readers), :] = weighted(taps, field, t)
        return carry

    lax.fori_loop(0, groups, body, 0)


def write_tiles(kernel, scalars, pieces, out, out_shape, start, flops):
    readers, _, per_tile, width = pieces[0].shape
    steps = out_shape[1]
    offset = start // LANES
    per_row = TS // LANES

    def piece_spec(piece):
        return pl.BlockSpec(
            (readers, piece.shape[1], per_tile, LANES), lambda i: (0, 0, 0, i)
        )

    in_specs = [pl.BlockSpec(memory_space=pltpu.SMEM) for _ in scalars]
    in_specs += [piece_spec(p) for p in pieces]
    operands = [*scalars, *pieces]
    aliases = {}
    if out is not None:
        in_specs.append(pl.BlockSpec(memory_space=pl.ANY))
        aliases = {len(operands): 0}
        operands.append(out)
    elements = readers * per_tile * width
    moved = steps + sum(p.shape[1] for p in pieces)
    return pl.pallas_call(
        functools.partial(kernel, readers, per_tile // SUBLANES),
        grid=(width // LANES,),
        out_shape=jax.ShapeDtypeStruct(out_shape, jnp.float32),
        in_specs=in_specs,
        out_specs=pl.BlockSpec(
            (1, steps, TS, LANES),
            lambda i: ((i + offset) // per_row, 0, 0, (i + offset) % per_row),
        ),
        input_output_aliases=aliases,
        cost_estimate=pl.CostEstimate(
            flops=flops * steps * elements, bytes_accessed=4 * moved * elements, transcendentals=0
        ),
    )(*operands)


def on_device(frames, taps):
    steps, _, strip, columns = frames.shape
    readers = lax.axis_size("sa")
    count = lax.axis_size("ta")
    per_tile = TS // readers
    tile_rows = strip // per_tile
    owned = tile_rows * (columns // TS) // readers
    span = owned * TS
    groups = columns // span
    out_shape = (owned, steps, TS, TS)
    up = [(i, i + 1) for i in range(count - 1)]
    down = [(i + 1, i) for i in range(count - 1)]
    swap = functools.partial(
        lax.all_to_all, axis_name="sa", split_axis=0, concat_axis=0, tiled=True
    )
    early, late = chunk_bounds(span)

    sides = []
    for start, stop in early:
        tail, head = raw_chunk(frames, span, start, stop - start)
        before = lax.ppermute(tail, "ta", up)
        after = lax.ppermute(head, "ta", down)
        sides.append((before, after))

    exchanged = []
    for start, stop in late:
        first, middle, last = pack_chunk(frames, readers, per_tile, span, start, stop - start)
        middle = swap(middle)
        before_mid = lax.ppermute(middle, "ta", up)
        after_mid = lax.ppermute(middle, "ta", down)
        first = swap(first)
        after_first = lax.ppermute(first, "ta", down)
        last = swap(last)
        before_last = lax.ppermute(last, "ta", up)
        exchanged.append(
            (first, middle, last, before_mid, before_last, after_first, after_mid)
        )

    out = None
    if early:
        packed = None
        width = early[-1][1] - early[0][0]
        shape = (tile_rows, groups, steps, per_tile, width)
        for (start, stop), (before, after) in zip(early, sides):
            packed = early_chunk(
                taps, frames, before, after, packed, shape, start, start - early[0][0]
            )
        packed = swap(packed.reshape(readers, steps, per_tile, width))
        out = write_tiles(place_kernel, (), (packed,), None, out_shape, early[0][0], 1)
    for (start, stop), pieces in zip(late, exchanged):
        out = write_tiles(smooth_kernel, (taps,), pieces, out, out_shape, start, 14)
    return out


def solution(mesh):
    placed = (P("ta", "sa", None, None), P())

    return jax.shard_map(
        on_device, mesh=mesh, in_specs=placed, out_specs=P("sa", "ta", None, None), check_vma=False
    )
```
